32 devices in a mesh: dp: 2 (over x), tp: 16 (over y, z, core).
Axes of the slice: x: 2, y: 2, z: 4, core: 2. Of those that a mesh axis runs over, the one named last changes fastest.
Arguments:
- x: bfloat16 [4096, 8192], P('dp'), parts along dimension 0
- w_gate: bfloat16 [8192, 32768], P(None, 'tp')
- w_up: bfloat16 [8192, 32768], P(None, 'tp')
- w_down: bfloat16 [32768, 8192], P('tp')
Outputs:
- output: bfloat16 [4096, 8192], P('dp'), parts along dimension 0
There are 2 independent parts. The reference program is written for one: setup_inputs(seed, part) draws one part's arguments, and reference() takes and returns one part's arrays. A program takes and returns all parts, laid end to end along the dimension named above; an argument that names none is the same for every part.
All inputs are finite; a program needn't handle non-finite values.
Results may differ from the reference program's by a relative error of at most 0.016.
Values are sent between devices in bfloat16 or wider.
A program may use at most 2 GiB of HBM per device.

```python
import jax
import jax.numpy as jnp

ROWS = 2048
D = 8192
FF = 32768


def setup_inputs(seed: int = 0, part: int = 0) -> dict:
    kx, kg, ku, kd = jax.random.split(jax.random.key(seed), 4)
    drawn = {
        "x": jax.random.normal(jax.random.fold_in(kx, part), (ROWS, D), jnp.float32),
        "w_gate": jax.random.normal(kg, (D, FF), jnp.float32) * D**-0.5,
        "w_up": jax.random.normal(ku, (D, FF), jnp.float32) * D**-0.5,
        "w_down": jax.random.normal(kd, (FF, D), jnp.float32) * FF**-0.5,
    }
    return {k: v.astype(jnp.bfloat16) for k, v in drawn.items()}


def reference(x, w_gate, w_up, w_down):
    gate = jnp.dot(x, w_gate, preferred_element_type=jnp.float32)
    up = jnp.dot(x, w_up, preferred_element_type=jnp.float32)
    hidden = (jax.nn.silu(gate) * up).astype(jnp.bfloat16)
    return jnp.dot(hidden, w_down, preferred_element_type=jnp.float32).astype(jnp.bfloat16)
```

```python
import jax
import jax.numpy as jnp
from jax import lax
from jax.experimental import pallas as pl
from jax.experimental.pallas import tpu as pltpu
from jax.sharding import PartitionSpec as P

ROWS, D, HID = 2048, 8192, 2048
R = 512
CW = 1024
HALF = D // 2
NQ = HALF // CW
CHUNKS = ROWS // R
PAIRS = CHUNKS * NQ
TN = 256
UNITS = HID // TN
NS = 4
B = 64
SLOTS = 6
LEAD = UNITS // 2
OFF = dict(A1e=3, A1m=6, A2m=9, A3m=11, A3e=15, A4e=16, B1m=4, B2m=8, B3m=10, B4m=14, B5m=13, B6m=17, Ce=23, Cm=22)
NIT = LEAD + PAIRS + (SLOTS - 1 + max(OFF.values())) // SLOTS
F32, BF16 = jnp.float32, jnp.bfloat16


def kernel(x, wg, wu, wd, y, xb, gb, ub, hb, wdb, dsend, drecv, sf, sb, r_ya, r_oa, r_xa, r_ob, r_xb, r_yb,
           s_x, s_w, s_wd, s_ds, s_dr, credit, q_rs, q_ss, q_ga, q_gb, q_f, q_loc, q_fw, q_sib):
    dp, t = lax.axis_index("dp"), lax.axis_index("tp")
    core, z, yy = t % 2, (t // 2) % 4, t // 8
    s = z // 2
    mid = (z == 1) | (z == 2)
    end = (z == 0) | (z == 3)

    def tid(a, b, c):
        return (dp, (a * 4 + b) * 2 + c)

    to_y, to_x, to_s = tid(1 - yy, z, core), tid(yy, 3 - z, core), tid(yy, z, 1 - core)
    to_io = tid(yy, z + 1 - 2 * (z % 2), core)

    def rcopy(src, dst, ssem, rsem, dev):
        return pltpu.make_async_remote_copy(
            src_ref=src, dst_ref=dst, send_sem=ssem, recv_sem=rsem, device_id=dev, device_id_type=pl.DeviceIdType.MESH)

    bar = pltpu.get_barrier_semaphore()
    for dev in (to_y, to_io, to_s):
        pl.semaphore_signal(bar, inc=1, device_id=dev, device_id_type=pl.DeviceIdType.MESH)

    @pl.when(mid)
    def _():
        pl.semaphore_signal(bar, inc=1, device_id=to_x, device_id_type=pl.DeviceIdType.MESH)
        pl.semaphore_wait(bar, 4)

    @pl.when(end)
    def _():
        pl.semaphore_wait(bar, 3)

    def rows(r0, n):
        return pl.ds(pl.multiple_of(r0, B), n)

    def x_copy(c):
        return pltpu.make_async_copy(x.at[rows(c * R, R), :], xb, s_x)

    def w_copies(u):
        b, n = u % 2, pl.ds(pl.multiple_of((u % UNITS) * TN, TN), TN)
        return (pltpu.make_async_copy(wg.at[:, n], gb.at[b], s_w.at[b, 0]),
                pltpu.make_async_copy(wu.at[:, n], ub.at[b], s_w.at[b, 1]))

    def wd_copy(k, half, p):
        n = pl.ds(pl.multiple_of(half * HALF + (p % NQ) * CW, CW), CW)
        return pltpu.make_async_copy(wd.at[:, n], wdb.at[k], s_wd.at[k])

    def gate_up(u, strip):
        b, n = u % 2, pl.ds(pl.multiple_of((u % UNITS) * TN, TN), TN)
        r = pl.ds(strip * (R // 2), R // 2)
        xv = xb[r, :]
        g = jnp.dot(xv, gb[b], preferred_element_type=F32)
        up = jnp.dot(xv, ub[b], preferred_element_type=F32)
        hb[(u // UNITS) % 2, r, n] = (jax.nn.silu(g) * up).astype(BF16)

    def swap(q):
        return rcopy(dsend, drecv.at[q % 2], s_ds, s_dr.at[q % 2], to_s)

    def term_for_other(q):
        for j in range(2):
            n = pl.ds(j * (CW // 2), CW // 2)
            dsend[:, n] = jnp.dot(hb[(q // NQ) % 2], wdb[0, :, n], preferred_element_type=F32).astype(BF16)

    def own_term(p, sl):
        for j in range(2):
            n = pl.ds(j * (CW // 2), CW // 2)
            v = jnp.dot(hb[(p // NQ) % 2], wdb[1, :, n], preferred_element_type=F32) + drecv[p % 2, :, n].astype(F32)
            sf[sl, :, n] = v
            sb[sl, :, n] = v.astype(BF16)

    def add(sl, r0, n, srcs):
        def strip(i, _):
            v = sf[sl, pl.ds(pl.multiple_of(r0 + i * 16, 16), 16), :]
            for ref, q0 in srcs:
                v = v + ref[sl, pl.ds(pl.multiple_of(q0 + i * 16, 16), 16), :].astype(F32)
            sb[sl, pl.ds(pl.multiple_of(r0 + i * 16, 16), 16), :] = v.astype(BF16)
            return 0
        lax.fori_loop(0, n // 16, strip, 0)

    ya, oa, xa, ob, xbl, yb = range(6)

    def reduce_copy(kind, sl, r0, n, dev):
        dst = (r_ya, r_oa, r_xa, r_ob, r_xb, r_yb)[kind].at[sl]
        return rcopy(sb.at[sl, rows(r0, n), :], dst, q_ss.at[sl, kind], q_rs.at[sl, kind], dev)

    def y_at(p, r0, n):
        col = pl.multiple_of(core * HALF + (p % NQ) * CW, CW)
        return y.at[rows((p // NQ) * R + r0, n), pl.ds(col, CW)]

    def block_a(a, b):
        return (a * 2 + b) * B

    def block_b(b, a):
        return 256 + (b * 2 + a) * B

    def recv_sem(sl, r0):
        return q_ga.at[sl, r0 // B]

    def local_final(p, sl, r0, k):
        return pltpu.make_async_copy(sb.at[sl, rows(r0, B), :], y_at(p, r0, B), q_loc.at[sl, k])

    def send_final(p, sl, r0, k, dev):
        return rcopy(sb.at[sl, rows(r0, B), :], y_at(p, r0, B), q_f.at[sl, k], recv_sem(sl, r0), dev)

    def forward(p, sl, r0, k, dev):
        return rcopy(y_at(p, r0, B), y_at(p, r0, B), q_fw.at[sl, k], recv_sem(sl, r0), dev)

    def sibling(p):
        return rcopy(y_at(p, 0, R), y_at(p, 0, R), q_sib.at[0, p], q_sib.at[1, p], to_s)

    def first(p, sl):
        reduce_copy(ya, sl, (1 - yy) * 128, 128, to_y).start()

        @pl.when(end)
        def _():
            reduce_copy(ob, sl, 256, 256, to_io).start()

    def e_a1e(p, sl):
        reduce_copy(ya, sl, 0, 128, to_y).wait_recv()
        add(sl, yy * 128, 128, [(r_ya, 0)])
        reduce_copy(oa, sl, yy * 128, 128, to_io).start()

    def e_a1m(p, sl):
        reduce_copy(ya, sl, 0, 128, to_y).wait_recv()
        reduce_copy(oa, sl, 0, 128, to_io).wait_recv()
        add(sl, block_a(yy, 1 - s), B, [(r_ya, (1 - s) * B), (r_oa, (1 - s) * B)])
        reduce_copy(xa, sl, block_a(yy, 1 - s), B, to_x).start()

    def finals(p, sl, r0, k):
        local_final(p, sl, r0, k).start()
        for i, dev in enumerate((to_io, to_x, to_y)):
            send_final(p, sl, r0, k * 3 + i, dev).start()

    def e_a2m(p, sl):
        reduce_copy(xa, sl, 0, B, to_x).wait_recv()
        add(sl, block_a(yy, s), B, [(r_ya, s * B), (r_oa, s * B), (r_xa, 0)])
        finals(p, sl, block_a(yy, s), 0)

    def arrived(p, sl, r0):
        forward(p, sl, r0, 0, to_y).wait_recv()

    def e_a3m(p, sl):
        r0 = block_a(yy, 1 - s)
        arrived(p, sl, r0)
        forward(p, sl, r0, 0, to_io).start()
        forward(p, sl, r0, 1, to_y).start()

    def e_a3e(p, sl):
        r0 = block_a(yy, s)
        arrived(p, sl, r0)
        forward(p, sl, r0, 0, to_y).start()

    def e_a4e(p, sl):
        r0 = block_a(yy, 1 - s)
        arrived(p, sl, r0)
        forward(p, sl, r0, 1, to_y).start()

    def e_b1m(p, sl):
        reduce_copy(ob, sl, 256, 256, to_io).wait_recv()
        add(sl, block_b(1 - s, 0), 128, [(r_ob, (1 - s) * 128)])
        reduce_copy(xbl, sl, block_b(1 - s, 0), 128, to_x).start()

    def e_b2m(p, sl):
        reduce_copy(xbl, sl, 256, 128, to_x).wait_recv()
        add(sl, block_b(s, 1 - yy), B, [(r_ob, (s * 2 + 1 - yy) * B), (r_xb, (1 - yy) * B)])
        reduce_copy(yb, sl, block_b(s, 1 - yy), B, to_y).start()

    def e_b3m(p, sl):
        reduce_copy(yb, sl, 256, B, to_y).wait_recv()
        add(sl, block_b(s, yy), B, [(r_ob, (s * 2 + yy) * B), (r_xb, yy * B), (r_yb, 0)])
        finals(p, sl, block_b(s, yy), 1)

    def e_b4m(p, sl):
        r0 = block_b(s, 1 - yy)
        arrived(p, sl, r0)
        forward(p, sl, r0, 2, to_x).start()
        forward(p, sl, r0, 3, to_io).start()

    def e_b5m(p, sl):
        r0 = block_b(1 - s, yy)
        arrived(p, sl, r0)
        forward(p, sl, r0, 4, to_io).start()

    def e_b6m(p, sl):
        r0 = block_b(1 - s, 1 - yy)
        arrived(p, sl, r0)
        forward(p, sl, r0, 5, to_io).start()

    def e_cm(p, sl):
        for b in range(2):
            arrived(p, sl, block_a(1 - yy, b))
        for k in range(2):
            local_final(p, sl, 0, k).wait()
        for k in range(6):
            send_final(p, sl, 0, k, to_y).wait_send()
            forward(p, sl, 0, k, to_y).wait_send()
        for kind, n in ((ya, 128), (xa, B), (xbl, 128), (yb, B)):
            reduce_copy(kind, sl, 0, n, to_y).wait_send()
        sibling(p).start()

    def e_ce(p, sl):
        for b in range(2):
            arrived(p, sl, block_a(1 - yy, b))
        for b in range(4):
            arrived(p, sl, 256 + b * B)
        for k in range(2):
            forward(p, sl, 0, k, to_y).wait_send()
        for kind, n in ((ya, 128), (ob, 256), (oa, 128)):
            reduce_copy(kind, sl, 0, n, to_y).wait_send()
        sibling(p).start()

    events = dict(A1e=(end, e_a1e), A1m=(mid, e_a1m), A2m=(mid, e_a2m), A3m=(mid, e_a3m), A3e=(end, e_a3e), A4e=(end, e_a4e),
                  B1m=(mid, e_b1m), B2m=(mid, e_b2m), B3m=(mid, e_b3m), B4m=(mid, e_b4m), B5m=(mid, e_b5m), B6m=(mid, e_b6m),
                  Ce=(end, e_ce), Cm=(mid, e_cm))

    def comm(it, j):
        for k in sorted(OFF, key=lambda k: -OFF[k]):
            if (OFF[k] + SLOTS - 1 - j) % SLOTS:
                continue
            p = it - LEAD - (OFF[k] + SLOTS - 1 - j) // SLOTS
            role, run = events[k]

            @pl.when((p >= 0) & (p < PAIRS) & role)
            def _():
                run(p, p % NS)

    x_copy(0).start()
    for c in w_copies(0):
        c.start()

    def body(it, _):
        for half in range(2):
            u = 2 * it + half
            for strip in range(2):
                @pl.when(it < PAIRS)
                def _():
                    if strip == 0:
                        if half == 0:
                            pl.when(it % LEAD == 0)(x_copy(0).wait)
                        for c in w_copies(u):
                            c.wait()

                        @pl.when(u + 1 < 2 * PAIRS)
                        def _():
                            for c in w_copies(u + 1):
                                c.start()
                    gate_up(u, strip)
                    if half == 1 and strip == 1:
                        pl.when((it % LEAD == LEAD - 1) & (it < PAIRS - 1))(lambda: x_copy(it // LEAD + 1).start())
                comm(it, half * 2 + strip)
        p, q = it - LEAD, it - LEAD + 1

        @pl.when((q >= 0) & (q < PAIRS))
        def _():
            wd_copy(0, 0, 0).wait()
            pl.when(q >= 1)(lambda: swap(q - 1).wait_send())
            term_for_other(q)
            pl.when(q >= 2)(lambda: pl.semaphore_wait(credit, 1))
            swap(q).start()

        @pl.when((q + 1 >= 0) & (q + 1 < PAIRS))
        def _():
            wd_copy(0, 1 - core, q + 1).start()
        comm(it, 4)

        @pl.when((p >= 0) & (p < PAIRS))
        def _():
            wd_copy(1, 0, 0).wait()
            swap(p).wait_recv()
            own_term(p, p % NS)

            @pl.when(p < PAIRS - 2)
            def _():
                pl.semaphore_signal(credit, inc=1, device_id=to_s, device_id_type=pl.DeviceIdType.MESH)
            first(p, p % NS)

        @pl.when((p + 1 >= 0) & (p + 1 < PAIRS))
        def _():
            wd_copy(1, core, p + 1).start()
        comm(it, 5)
        return 0

    lax.fori_loop(0, NIT, body, 0)
    swap(PAIRS - 1).wait_send()

    def last(p, _):
        sibling(p).wait()
        return 0

    lax.fori_loop(0, PAIRS, last, 0)


def solution(mesh):
    def step(x, w_gate, w_up, w_down):
        any_ = pl.BlockSpec(memory_space=pl.ANY)
        dma = pltpu.SemaphoreType.DMA
        flops = 6 * ROWS * D * HID
        return pl.pallas_call(
            kernel,
            out_shape=jax.ShapeDtypeStruct((ROWS, D), BF16),
            in_specs=[any_] * 4,
            out_specs=any_,
            scratch_shapes=[
                pltpu.VMEM((R, D), BF16),
                pltpu.VMEM((2, D, TN), BF16),
                pltpu.VMEM((2, D, TN), BF16),
                pltpu.VMEM((2, R, HID), BF16),
                pltpu.VMEM((2, HID, CW), BF16),
                pltpu.VMEM((R, CW), BF16),
                pltpu.VMEM((2, R, CW), BF16),
                pltpu.VMEM((NS, R, CW), F32),
                pltpu.VMEM((NS, R, CW), BF16),
                pltpu.VMEM((NS, 2 * B, CW), BF16),
                pltpu.VMEM((NS, 2 * B, CW), BF16),
                pltpu.VMEM((NS, B, CW), BF16),
                pltpu.VMEM((NS, 4 * B, CW), BF16),
                pltpu.VMEM((NS, 2 * B, CW), BF16),
                pltpu.VMEM((NS, B, CW), BF16),
                dma,
                dma((2, 2)),
                dma((2,)),
                dma,
                dma((2,)),
                pltpu.SemaphoreType.REGULAR,
                dma((NS, 6)),
                dma((NS, 6)),
                dma((NS, 8)),
                dma((1,)),
                dma((NS, 6)),
                dma((NS, 2)),
                dma((NS, 6)),
                dma((2, PAIRS)),
            ],
            compiler_params=pltpu.CompilerParams(
                collective_id=0, has_side_effects=True, vmem_limit_bytes=67043328),
            cost_estimate=pl.CostEstimate(flops=flops, bytes_accessed=1 << 29, transcendentals=ROWS * HID),
            name="mlp",
        )(x, w_gate, w_up, w_down)

    return jax.shard_map(
        step,
        mesh=mesh,
        in_specs=(P("dp", None), P(None, "tp"), P(None, "tp"), P("tp", None)),
        out_specs=P("dp", None),
        check_vma=False,
    )
```

```python
import jax
import jax.numpy as jnp
from jax import lax
from jax.experimental import pallas as pl
from jax.experimental.pallas import tpu as pltpu
from jax.sharding import PartitionSpec as P

ROWS, D, HID = 2048, 8192, 2048
R = 512
CW = 512
HALF = D // 2
NQ = HALF // CW
CHUNKS = ROWS // R
PAIRS = CHUNKS * NQ
TN = 256
UNITS = HID // TN
NS = 8
B = 64
SLOTS = 4
LEAD = UNITS
OFF = dict(Cm=29, B5m=20, A1e=3, B1m=7, A1m=8, A3e=15, A3m=20, B4m=20, B8e=22, Ce=28, B2m=11, A2m=13, A4e=22, B3m=14, B7e=16)
NIT = LEAD + PAIRS + max(OFF.values()) // SLOTS
F32, BF16 = jnp.float32, jnp.bfloat16


def kernel(x, wg, wu, wd, y, xb, gb, ub, hb, wdb, dsend, drecv, sf, sb, r_ya, r_oa, r_xa, r_ob, r_xb, r_yb,
           s_x, s_w, s_wd, s_ds, s_dr, credit, q_rs, q_send, q_final, q_leaf, q_sib):
    dp, t = lax.axis_index("dp"), lax.axis_index("tp")
    core, z, yy = t % 2, (t // 2) % 4, t // 8
    s = z // 2
    mid = (z == 1) | (z == 2)
    end = (z == 0) | (z == 3)

    def tid(a, b, c):
        return (dp, (a * 4 + b) * 2 + c)

    to_y, to_x, to_s = tid(1 - yy, z, core), tid(yy, 3 - z, core), tid(yy, z, 1 - core)
    to_io = tid(yy, z + 1 - 2 * (z % 2), core)

    def rcopy(src, dst, ssem, rsem, dev):
        return pltpu.make_async_remote_copy(
            src_ref=src, dst_ref=dst, send_sem=ssem, recv_sem=rsem, device_id=dev, device_id_type=pl.DeviceIdType.MESH)

    bar = pltpu.get_barrier_semaphore()
    for dev in (to_y, to_io, to_s):
        pl.semaphore_signal(bar, inc=1, device_id=dev, device_id_type=pl.DeviceIdType.MESH)

    @pl.when(mid)
    def _():
        pl.semaphore_signal(bar, inc=1, device_id=to_x, device_id_type=pl.DeviceIdType.MESH)
        pl.semaphore_wait(bar, 4)

    @pl.when(end)
    def _():
        pl.semaphore_wait(bar, 3)

    def rows(r0, n):
        return pl.ds(pl.multiple_of(r0, B), n)

    def x_copy(c, i):
        h = R // 2
        return pltpu.make_async_copy(x.at[rows(c * R + i * h, h), :], xb.at[pl.ds(i * h, h), :], s_x.at[i])

    def w_copies(u):
        b, n = u % 2, pl.ds(pl.multiple_of((u % UNITS) * TN, TN), TN)
        return (pltpu.make_async_copy(wg.at[:, n], gb.at[b], s_w.at[b, 0]),
                pltpu.make_async_copy(wu.at[:, n], ub.at[b], s_w.at[b, 1]))

    def wd_copy(k, half, p):
        n = pl.ds(pl.multiple_of(half * HALF + (p % NQ) * CW, CW), CW)
        return pltpu.make_async_copy(wd.at[:, n], wdb.at[k], s_wd.at[k])

    def gate_up(u, i):
        b, n = u % 2, pl.ds(pl.multiple_of((u % UNITS) * TN, TN), TN)
        r = pl.ds(i * (R // 2), R // 2)
        g = jnp.dot(xb[r, :], gb[b], preferred_element_type=F32)
        up = jnp.dot(xb[r, :], ub[b], preferred_element_type=F32)
        hb[(u // UNITS) % 2, r, n] = (jax.nn.silu(g) * up).astype(BF16)

    def swap(q):
        return rcopy(dsend, drecv.at[q % 2], s_ds, s_dr.at[q % 2], to_s)

    def term_for_other(q):
        for j in range(1):
            n = pl.ds(j * CW, CW)
            dsend[:, n] = jnp.dot(hb[(q // NQ) % 2], wdb[0, :, n], preferred_element_type=F32).astype(BF16)

    def own_term(p, sl):
        for j in range(1):
            n = pl.ds(j * CW, CW)
            v = jnp.dot(hb[(p // NQ) % 2], wdb[1, :, n], preferred_element_type=F32) + drecv[p % 2, :, n].astype(F32)
            sf[sl, :, n] = v
            sb[sl, :, n] = v.astype(BF16)

    def add(sl, r0, n, srcs):
        w = 32
        def strip(i, _):
            v = sf[sl, pl.ds(pl.multiple_of(r0 + i * w, w), w), :]
            for ref, q0 in srcs:
                v = v + ref[sl, pl.ds(pl.multiple_of(q0 + i * w, w), w), :].astype(F32)
            sb[sl, pl.ds(pl.multiple_of(r0 + i * w, w), w), :] = v.astype(BF16)
            return 0
        lax.fori_loop(0, n // w, strip, 0, unroll=True)

    ya, oa, xa, ob, xbl, yb = range(6)

    def reduce_copy(kind, sl, r0, n, dev):
        dst = (r_ya, r_oa, r_xa, r_ob, r_xb, r_yb)[kind].at[sl]
        return rcopy(sb.at[sl, rows(r0, n), :], dst, q_send.at[sl], q_rs.at[sl, kind], dev)

    def y_at(p, r0, n):
        col = pl.multiple_of(core * HALF + (p % NQ) * CW, CW)
        return y.at[rows((p // NQ) * R + r0, n), pl.ds(col, CW)]

    def block_a(a, b):
        return (a * 2 + b) * B

    def block_b(b, a):
        return 256 + (b * 2 + a) * B

    def final_sem(sl, r0):
        return q_final.at[sl, r0 // B]

    def local_final(p, sl, r0):
        return pltpu.make_async_copy(sb.at[sl, rows(r0, B), :], y_at(p, r0, B), q_send.at[sl])

    def send_final(p, sl, r0, dev, leaf=False):
        sem = q_leaf.at[sl] if leaf else final_sem(sl, r0)
        return rcopy(sb.at[sl, rows(r0, B), :], y_at(p, r0, B), q_send.at[sl], sem, dev)

    def forward(p, sl, r0, dev, leaf=False):
        sem = q_leaf.at[sl] if leaf else final_sem(sl, r0)
        return rcopy(y_at(p, r0, B), y_at(p, r0, B), q_send.at[sl], sem, dev)

    def wait_blocks(sem, n):
        part = y.at[pl.ds(0, n * B), pl.ds(0, CW)]
        pltpu.make_async_copy(part, part, sem).wait()

    def sibling(p):
        return rcopy(y_at(p, 0, R), y_at(p, 0, R), q_sib.at[0, p], q_sib.at[1, p], to_s)

    def first(p, sl):
        reduce_copy(ya, sl, (1 - yy) * 128, 128, to_y).start()

        @pl.when(end)
        def _():
            reduce_copy(ob, sl, 256, 256, to_io).start()

    def e_a1e(p, sl):
        reduce_copy(ya, sl, 0, 128, to_y).wait_recv()
        add(sl, yy * 128, 128, [(r_ya, 0)])
        reduce_copy(oa, sl, yy * 128, 128, to_io).start()

    def e_a1m(p, sl):
        reduce_copy(ya, sl, 0, 128, to_y).wait_recv()
        reduce_copy(oa, sl, 0, 128, to_io).wait_recv()
        add(sl, block_a(yy, 1 - s), B, [(r_ya, (1 - s) * B), (r_oa, (1 - s) * B)])
        reduce_copy(xa, sl, block_a(yy, 1 - s), B, to_x).start()

    def finals(p, sl, r0, leaf):
        send_final(p, sl, r0, to_x).start()
        send_final(p, sl, r0, to_io).start()
        send_final(p, sl, r0, to_y, leaf).start()
        local_final(p, sl, r0).start()

    def e_a2m(p, sl):
        reduce_copy(xa, sl, 0, B, to_x).wait_recv()
        add(sl, block_a(yy, s), B, [(r_ya, s * B), (r_oa, s * B), (r_xa, 0)])
        finals(p, sl, block_a(yy, s), True)

    def arrived(p, sl, r0):
        forward(p, sl, r0, to_y).wait_recv()

    def e_a3m(p, sl):
        r0 = block_a(yy, 1 - s)
        arrived(p, sl, r0)
        forward(p, sl, r0, to_io).start()
        forward(p, sl, r0, to_y, True).start()

    def pass_across(r0):
        def run(p, sl):
            arrived(p, sl, r0)
            forward(p, sl, r0, to_y, True).start()
        return run

    e_a3e, e_a4e = pass_across(block_a(yy, s)), pass_across(block_a(yy, 1 - s))
    e_b7e, e_b8e = pass_across(block_b(s, yy)), pass_across(block_b(1 - s, yy))

    def e_b1m(p, sl):
        reduce_copy(ob, sl, 256, 256, to_io).wait_recv()
        add(sl, block_b(1 - s, 0), 128, [(r_ob, (1 - s) * 128)])
        reduce_copy(xbl, sl, block_b(1 - s, 0), 128, to_x).start()

    def e_b2m(p, sl):
        reduce_copy(xbl, sl, 256, 128, to_x).wait_recv()
        add(sl, block_b(s, 1 - yy), B, [(r_ob, (s * 2 + 1 - yy) * B), (r_xb, (1 - yy) * B)])
        reduce_copy(yb, sl, block_b(s, 1 - yy), B, to_y).start()

    def e_b3m(p, sl):
        reduce_copy(yb, sl, 256, B, to_y).wait_recv()
        add(sl, block_b(s, yy), B, [(r_ob, (s * 2 + yy) * B), (r_xb, yy * B), (r_yb, 0)])
        finals(p, sl, block_b(s, yy), False)

    def e_b4m(p, sl):
        r0 = block_b(s, 1 - yy)
        arrived(p, sl, r0)
        forward(p, sl, r0, to_x, True).start()

    def e_b5m(p, sl):
        r0 = block_b(1 - s, yy)
        arrived(p, sl, r0)
        forward(p, sl, r0, to_io).start()

    def e_cm(p, sl):
        wait_blocks(q_leaf.at[sl], 3)
        wait_blocks(q_send.at[sl], 18)
        sibling(p).start()

    def e_ce(p, sl):
        wait_blocks(q_leaf.at[sl], 4)
        wait_blocks(q_send.at[sl], 12)
        sibling(p).start()

    events = dict(A1e=(end, e_a1e), A1m=(mid, e_a1m), A2m=(mid, e_a2m), A3m=(mid, e_a3m), A3e=(end, e_a3e), A4e=(end, e_a4e),
                  B1m=(mid, e_b1m), B2m=(mid, e_b2m), B3m=(mid, e_b3m), B4m=(mid, e_b4m), B5m=(mid, e_b5m), B7e=(end, e_b7e), B8e=(end, e_b8e),
                  Ce=(end, e_ce), Cm=(mid, e_cm))

    def comm(it, j):
        here = [(OFF[k], OFF[k] // SLOTS, *events[k]) for k in sorted(OFF, key=lambda k: -OFF[k]) if OFF[k] % SLOTS == j]
        if not here:
            return
        lags = [e[1] for e in here]
        steady = (it >= LEAD + max(lags)) & (it < LEAD + PAIRS + min(lags))

        def run_all(role, guarded):
            for _, lag, of, run in here:
                if of is not role:
                    continue
                p = it - LEAD - lag
                if guarded:
                    pl.when((p >= 0) & (p < PAIRS))(lambda run=run, p=p: run(p, p % NS))
                else:
                    run(p, p % NS)

        def both(guarded):
            lax.cond(mid, lambda: run_all(mid, guarded), lambda: run_all(end, guarded))

        lax.cond(steady, lambda: both(False), lambda: both(True))

    x_copy(0, 0).start()
    for c in w_copies(0):
        c.start()
    x_copy(0, 1).start()

    def other_half(q):
        wd_copy(0, 0, 0).wait()
        pl.when(q >= 1)(lambda: swap(q - 1).wait_send())
        term_for_other(q)
        pl.when(q >= 2)(lambda: pl.semaphore_wait(credit, 1))
        swap(q).start()
        pl.when(q + 1 < PAIRS)(lambda: wd_copy(0, 1 - core, q + 1).start())

    def body(it, _):
        p, q = it - LEAD, it - LEAD + 1

        @pl.when((p >= 0) & (p < PAIRS))
        def _():
            wd_copy(1, 0, 0).wait()
            swap(p).wait_recv()
            own_term(p, p % NS)

            @pl.when(p < PAIRS - 2)
            def _():
                pl.semaphore_signal(credit, inc=1, device_id=to_s, device_id_type=pl.DeviceIdType.MESH)
            first(p, p % NS)
            pl.when(p + 1 < PAIRS)(lambda: wd_copy(1, core, p + 1).start())
        comm(it, 0)
        pl.when((q >= 1) & (q < PAIRS) & (q % NQ != 0))(lambda: other_half(q))
        comm(it, 1)
        for i in range(2):
            @pl.when(it < PAIRS)
            def _():
                pl.when(it % UNITS == 0)(x_copy(0, i).wait)
                if i == 0:
                    for c in w_copies(it):
                        c.wait()

                    @pl.when(it + 1 < PAIRS)
                    def _():
                        for c in w_copies(it + 1):
                            c.start()

                    @pl.when(it == 0)
                    def _():
                        wd_copy(0, 1 - core, 0).start()
                        wd_copy(1, core, 0).start()
                gate_up(it, i)
                pl.when((it % UNITS == UNITS - 1) & (it < PAIRS - 1))(lambda: x_copy(it // UNITS + 1, i).start())
            comm(it, 2 + i)
        pl.when((q >= 0) & (q < PAIRS) & (q % NQ == 0))(lambda: other_half(q))
        return 0

    lax.fori_loop(0, NIT, body, 0)
    swap(PAIRS - 1).wait_send()

    def last(p, _):
        sibling(p).wait()
        return 0

    lax.fori_loop(0, PAIRS, last, 0)


def copy_out(a, o, buf, si, so):
    n, r, steps = 8, ROWS // 16, 16

    def load(i):
        return pltpu.make_async_copy(a.at[pl.ds(i * r, r), :], buf.at[i % n], si.at[i % n])

    def store(i):
        return pltpu.make_async_copy(buf.at[i % n], o.at[pl.ds(i * r, r), :], so.at[i % n])

    for i in range(n // 2):
        load(i).start()
    for i in range(steps):
        load(i).wait()
        store(i).start()
        j = i + n // 2
        if j < steps:
            if j >= n:
                store(j - n).wait()
            load(j).start()
    for i in range(steps - n, steps):
        store(i).wait()


def solution(mesh):
    def step(x, w_gate, w_up, w_down):
        any_ = pl.BlockSpec(memory_space=pl.ANY)
        dma = pltpu.SemaphoreType.DMA
        flops = 6 * ROWS * D * HID
        y = pl.pallas_call(
            kernel,
            out_shape=jax.ShapeDtypeStruct((ROWS, D), BF16),
            in_specs=[any_] * 4,
            out_specs=any_,
            scratch_shapes=[
                pltpu.VMEM((R, D), BF16),
                pltpu.VMEM((2, D, TN), BF16),
                pltpu.VMEM((2, D, TN), BF16),
                pltpu.VMEM((2, R, HID), BF16),
                pltpu.VMEM((2, HID, CW), BF16),
                pltpu.VMEM((R, CW), BF16),
                pltpu.VMEM((2, R, CW), BF16),
                pltpu.VMEM((NS, R, CW), F32),
                pltpu.VMEM((NS, R, CW), BF16),
                pltpu.VMEM((NS, 2 * B, CW), BF16),
                pltpu.VMEM((NS, 2 * B, CW), BF16),
                pltpu.VMEM((NS, B, CW), BF16),
                pltpu.VMEM((NS, 4 * B, CW), BF16),
                pltpu.VMEM((NS, 2 * B, CW), BF16),
                pltpu.VMEM((NS, B, CW), BF16),
                dma((2,)),
                dma((2, 2)),
                dma((2,)),
                dma,
                dma((2,)),
                pltpu.SemaphoreType.REGULAR,
                dma((NS, 6)),
                dma((NS,)),
                dma((NS, 8)),
                dma((NS,)),
                dma((2, PAIRS)),
            ],
            compiler_params=pltpu.CompilerParams(
                collective_id=0, has_side_effects=True, vmem_limit_bytes=67043328),
            cost_estimate=pl.CostEstimate(flops=flops, bytes_accessed=1 << 29, transcendentals=ROWS * HID),
            name="mlp",
        )(x, w_gate, w_up, w_down)
        return pl.pallas_call(
            copy_out,
            out_shape=jax.ShapeDtypeStruct((ROWS, D), BF16),
            in_specs=[any_],
            out_specs=any_,
            scratch_shapes=[pltpu.VMEM((8, ROWS // 16, D), BF16), dma((8,)), dma((8,))],
            compiler_params=pltpu.CompilerParams(vmem_limit_bytes=60 << 20),
            cost_estimate=pl.CostEstimate(flops=0, bytes_accessed=4 * ROWS * D, transcendentals=0),
            name="copy_out",
        )(y)

    return jax.shard_map(
        step,
        mesh=mesh,
        in_specs=(P("dp", None), P(None, "tp"), P(None, "tp"), P("tp", None)),
        out_specs=P("dp", None),
        check_vma=False,
    )
```

```python
import jax
import jax.numpy as jnp
from jax import lax
from jax.experimental import pallas as pl
from jax.experimental.pallas import tpu as pltpu
from jax.sharding import PartitionSpec as P

ROWS, D, HID = 2048, 8192, 2048
R = 512
CW = 512
HALF = D // 2
NQ = HALF // CW
CHUNKS = ROWS // R
PAIRS = CHUNKS * NQ
TN = 256
UNITS = HID // TN
NS = 8
B = 64
SLOTS = 4
LEAD = UNITS
OFF = dict(Cm=29, B5m=20, A1e=3, B1m=7, A1m=8, A3e=15, A3m=20, B4m=20, B8e=22, Ce=28, B2m=11, A2m=13, A4e=22, B3m=14, B7e=16)
NIT = LEAD + PAIRS + max(OFF.values()) // SLOTS
KEEP = NIT - 7
F32, BF16 = jnp.float32, jnp.bfloat16


def kernel(x, wg, wu, wd, y, xb, gb, ub, hb, wdb, dsend, drecv, sf, sb, r_ya, r_oa, r_xa, r_ob, r_xb, r_yb,
           s_x, s_w, s_wd, s_ds, s_dr, credit, q_rs, q_send, q_final, q_leaf, q_sib, s_keep):
    dp, t = lax.axis_index("dp"), lax.axis_index("tp")
    core, z, yy = t % 2, (t // 2) % 4, t // 8
    s = z // 2
    mid = (z == 1) | (z == 2)
    end = (z == 0) | (z == 3)

    def tid(a, b, c):
        return (dp, (a * 4 + b) * 2 + c)

    to_y, to_x, to_s = tid(1 - yy, z, core), tid(yy, 3 - z, core), tid(yy, z, 1 - core)
    to_io = tid(yy, z + 1 - 2 * (z % 2), core)

    def rcopy(src, dst, ssem, rsem, dev):
        return pltpu.make_async_remote_copy(
            src_ref=src, dst_ref=dst, send_sem=ssem, recv_sem=rsem, device_id=dev, device_id_type=pl.DeviceIdType.MESH)

    bar = pltpu.get_barrier_semaphore()
    for dev in (to_y, to_io, to_s):
        pl.semaphore_signal(bar, inc=1, device_id=dev, device_id_type=pl.DeviceIdType.MESH)

    @pl.when(mid)
    def _():
        pl.semaphore_signal(bar, inc=1, device_id=to_x, device_id_type=pl.DeviceIdType.MESH)
        pl.semaphore_wait(bar, 4)

    @pl.when(end)
    def _():
        pl.semaphore_wait(bar, 3)

    def rows(r0, n):
        return pl.ds(pl.multiple_of(r0, B), n)

    def x_copy(c, i):
        h = R // 2
        return pltpu.make_async_copy(x.at[rows(c * R + i * h, h), :], xb.at[pl.ds(i * h, h), :], s_x.at[i])

    def w_copies(u):
        b, n = u % 2, pl.ds(pl.multiple_of((u % UNITS) * TN, TN), TN)
        return (pltpu.make_async_copy(wg.at[:, n], gb.at[b], s_w.at[b, 0]),
                pltpu.make_async_copy(wu.at[:, n], ub.at[b], s_w.at[b, 1]))

    def wd_copy(k, half, p):
        n = pl.ds(pl.multiple_of(half * HALF + (p % NQ) * CW, CW), CW)
        return pltpu.make_async_copy(wd.at[:, n], wdb.at[k], s_wd.at[k])

    def gate_up(u, i):
        b, n = u % 2, pl.ds(pl.multiple_of((u % UNITS) * TN, TN), TN)
        r = pl.ds(i * (R // 2), R // 2)
        g = jnp.dot(xb[r, :], gb[b], preferred_element_type=F32)
        up = jnp.dot(xb[r, :], ub[b], preferred_element_type=F32)
        hb[(u // UNITS) % 2, r, n] = (jax.nn.silu(g) * up).astype(BF16)

    def swap(q):
        return rcopy(dsend, drecv.at[q % 2], s_ds, s_dr.at[q % 2], to_s)

    def term_for_other(q):
        for j in range(1):
            n = pl.ds(j * CW, CW)
            dsend[:, n] = jnp.dot(hb[(q // NQ) % 2], wdb[0, :, n], preferred_element_type=F32).astype(BF16)

    def own_term(p, sl):
        for j in range(1):
            n = pl.ds(j * CW, CW)
            v = jnp.dot(hb[(p // NQ) % 2], wdb[1, :, n], preferred_element_type=F32) + drecv[p % 2, :, n].astype(F32)
            sf[sl, :, n] = v
            sb[sl, :, n] = v.astype(BF16)

    def add(sl, r0, n, srcs):
        w = 32
        def strip(i, _):
            v = sf[sl, pl.ds(pl.multiple_of(r0 + i * w, w), w), :]
            for ref, q0 in srcs:
                v = v + ref[sl, pl.ds(pl.multiple_of(q0 + i * w, w), w), :].astype(F32)
            sb[sl, pl.ds(pl.multiple_of(r0 + i * w, w), w), :] = v.astype(BF16)
            return 0
        lax.fori_loop(0, n // w, strip, 0, unroll=True)

    ya, oa, xa, ob, xbl, yb = range(6)

    def reduce_copy(kind, sl, r0, n, dev):
        dst = (r_ya, r_oa, r_xa, r_ob, r_xb, r_yb)[kind].at[sl]
        return rcopy(sb.at[sl, rows(r0, n), :], dst, q_send.at[sl], q_rs.at[sl, kind], dev)

    def y_at(p, r0, n):
        col = pl.multiple_of(core * HALF + (p % NQ) * CW, CW)
        return y.at[rows((p // NQ) * R + r0, n), pl.ds(col, CW)]

    def block_a(a, b):
        return (a * 2 + b) * B

    def block_b(b, a):
        return 256 + (b * 2 + a) * B

    def final_sem(sl, r0):
        return q_final.at[sl, r0 // B]

    def local_final(p, sl, r0):
        return pltpu.make_async_copy(sb.at[sl, rows(r0, B), :], y_at(p, r0, B), q_send.at[sl])

    def send_final(p, sl, r0, dev, leaf=False):
        sem = q_leaf.at[sl] if leaf else final_sem(sl, r0)
        return rcopy(sb.at[sl, rows(r0, B), :], y_at(p, r0, B), q_send.at[sl], sem, dev)

    def forward(p, sl, r0, dev, leaf=False):
        sem = q_leaf.at[sl] if leaf else final_sem(sl, r0)
        return rcopy(y_at(p, r0, B), y_at(p, r0, B), q_send.at[sl], sem, dev)

    def wait_blocks(sem, n):
        part = y.at[pl.ds(0, n * B), pl.ds(0, CW)]
        pltpu.make_async_copy(part, part, sem).wait()

    def sibling(p):
        return rcopy(y_at(p, 0, R), y_at(p, 0, R), q_sib.at[0, p], q_sib.at[1, p], to_s)

    def first(p, sl):
        reduce_copy(ya, sl, (1 - yy) * 128, 128, to_y).start()

        @pl.when(end)
        def _():
            reduce_copy(ob, sl, 256, 256, to_io).start()

    def e_a1e(p, sl):
        reduce_copy(ya, sl, 0, 128, to_y).wait_recv()
        add(sl, yy * 128, 128, [(r_ya, 0)])
        reduce_copy(oa, sl, yy * 128, 128, to_io).start()

    def e_a1m(p, sl):
        reduce_copy(ya, sl, 0, 128, to_y).wait_recv()
        reduce_copy(oa, sl, 0, 128, to_io).wait_recv()
        add(sl, block_a(yy, 1 - s), B, [(r_ya, (1 - s) * B), (r_oa, (1 - s) * B)])
        reduce_copy(xa, sl, block_a(yy, 1 - s), B, to_x).start()

    def finals(p, sl, r0, leaf):
        send_final(p, sl, r0, to_x).start()
        send_final(p, sl, r0, to_io).start()
        send_final(p, sl, r0, to_y, leaf).start()
        local_final(p, sl, r0).start()

    def e_a2m(p, sl):
        reduce_copy(xa, sl, 0, B, to_x).wait_recv()
        add(sl, block_a(yy, s), B, [(r_ya, s * B), (r_oa, s * B), (r_xa, 0)])
        finals(p, sl, block_a(yy, s), True)

    def arrived(p, sl, r0):
        forward(p, sl, r0, to_y).wait_recv()

    def e_a3m(p, sl):
        r0 = block_a(yy, 1 - s)
        arrived(p, sl, r0)
        forward(p, sl, r0, to_io).start()
        forward(p, sl, r0, to_y, True).start()

    def pass_across(r0):
        def run(p, sl):
            arrived(p, sl, r0)
            forward(p, sl, r0, to_y, True).start()
        return run

    e_a3e, e_a4e = pass_across(block_a(yy, s)), pass_across(block_a(yy, 1 - s))
    e_b7e, e_b8e = pass_across(block_b(s, yy)), pass_across(block_b(1 - s, yy))

    def e_b1m(p, sl):
        reduce_copy(ob, sl, 256, 256, to_io).wait_recv()
        add(sl, block_b(1 - s, 0), 128, [(r_ob, (1 - s) * 128)])
        reduce_copy(xbl, sl, block_b(1 - s, 0), 128, to_x).start()

    def e_b2m(p, sl):
        reduce_copy(xbl, sl, 256, 128, to_x).wait_recv()
        add(sl, block_b(s, 1 - yy), B, [(r_ob, (s * 2 + 1 - yy) * B), (r_xb, (1 - yy) * B)])
        reduce_copy(yb, sl, block_b(s, 1 - yy), B, to_y).start()

    def e_b3m(p, sl):
        reduce_copy(yb, sl, 256, B, to_y).wait_recv()
        add(sl, block_b(s, yy), B, [(r_ob, (s * 2 + yy) * B), (r_xb, yy * B), (r_yb, 0)])
        finals(p, sl, block_b(s, yy), False)

    def e_b4m(p, sl):
        r0 = block_b(s, 1 - yy)
        arrived(p, sl, r0)
        forward(p, sl, r0, to_x, True).start()

    def e_b5m(p, sl):
        r0 = block_b(1 - s, yy)
        arrived(p, sl, r0)
        forward(p, sl, r0, to_io).start()

    def e_cm(p, sl):
        wait_blocks(q_leaf.at[sl], 3)
        wait_blocks(q_send.at[sl], 18)
        sibling(p).start()

    def e_ce(p, sl):
        wait_blocks(q_leaf.at[sl], 4)
        wait_blocks(q_send.at[sl], 12)
        sibling(p).start()

    events = dict(A1e=(end, e_a1e), A1m=(mid, e_a1m), A2m=(mid, e_a2m), A3m=(mid, e_a3m), A3e=(end, e_a3e), A4e=(end, e_a4e),
                  B1m=(mid, e_b1m), B2m=(mid, e_b2m), B3m=(mid, e_b3m), B4m=(mid, e_b4m), B5m=(mid, e_b5m), B7e=(end, e_b7e), B8e=(end, e_b8e),
                  Ce=(end, e_ce), Cm=(mid, e_cm))

    def comm(it, j):
        here = [(OFF[k], OFF[k] // SLOTS, *events[k]) for k in sorted(OFF, key=lambda k: -OFF[k]) if OFF[k] % SLOTS == j]
        if not here:
            return
        lags = [e[1] for e in here]
        steady = (it >= LEAD + max(lags)) & (it < LEAD + PAIRS + min(lags))

        def run_all(role, guarded):
            for _, lag, of, run in here:
                if of is not role:
                    continue
                p = it - LEAD - lag
                if guarded:
                    pl.when((p >= 0) & (p < PAIRS))(lambda run=run, p=p: run(p, p % NS))
                else:
                    run(p, p % NS)

        def both(guarded):
            lax.cond(mid, lambda: run_all(mid, guarded), lambda: run_all(end, guarded))

        lax.cond(steady, lambda: both(False), lambda: both(True))

    x_copy(0, 0).start()
    for c in w_copies(0):
        c.start()
    x_copy(0, 1).start()

    def other_half(q):
        wd_copy(0, 0, 0).wait()
        pl.when(q >= 1)(lambda: swap(q - 1).wait_send())
        term_for_other(q)
        pl.when(q >= 2)(lambda: pl.semaphore_wait(credit, 1))
        swap(q).start()
        pl.when(q + 1 < PAIRS)(lambda: wd_copy(0, 1 - core, q + 1).start())

    def landed(p, _):
        sibling(p).wait_recv()
        return 0

    def body(it, _):
        p, q = it - LEAD, it - LEAD + 1

        @pl.when(it == KEEP)
        def _():
            lax.fori_loop(0, 3 * NQ, landed, 0)
            pltpu.make_async_copy(y.at[pl.ds(0, R), :], xb, s_keep.at[0]).start()
            for c, ref in ((1, gb), (2, ub)):
                for k in range(D // TN // 2):
                    for src, dst in kept(y, ref, k, c):
                        pltpu.make_async_copy(src, dst, s_keep.at[c]).start()


        @pl.when((p >= 0) & (p < PAIRS))
        def _():
            wd_copy(1, 0, 0).wait()
            swap(p).wait_recv()
            own_term(p, p % NS)

            @pl.when(p < PAIRS - 2)
            def _():
                pl.semaphore_signal(credit, inc=1, device_id=to_s, device_id_type=pl.DeviceIdType.MESH)
            first(p, p % NS)
            pl.when(p + 1 < PAIRS)(lambda: wd_copy(1, core, p + 1).start())
        comm(it, 0)
        pl.when((q >= 1) & (q < PAIRS) & (q % NQ != 0))(lambda: other_half(q))
        comm(it, 1)
        for i in range(2):
            @pl.when(it < PAIRS)
            def _():
                pl.when(it % UNITS == 0)(x_copy(0, i).wait)
                if i == 0:
                    for c in w_copies(it):
                        c.wait()

                    @pl.when(it + 1 < PAIRS)
                    def _():
                        for c in w_copies(it + 1):
                            c.start()

                    @pl.when(it == 0)
                    def _():
                        wd_copy(0, 1 - core, 0).start()
                        wd_copy(1, core, 0).start()
                gate_up(it, i)
                pl.when((it % UNITS == UNITS - 1) & (it < PAIRS - 1))(lambda: x_copy(it // UNITS + 1, i).start())
            comm(it, 2 + i)
        pl.when((q >= 0) & (q < PAIRS) & (q % NQ == 0))(lambda: other_half(q))
        return 0

    lax.fori_loop(0, NIT, body, 0)
    swap(PAIRS - 1).wait_send()

    pltpu.make_async_copy(y.at[pl.ds(0, R), :], xb, s_keep.at[0]).wait()
    for c in (1, 2):
        pltpu.make_async_copy(y.at[pl.ds(c * R, R), :], y.at[pl.ds(c * R, R), :], s_keep.at[c]).wait()

    def last(p, _):
        sibling(p).wait_send()
        pl.when(p >= 3 * NQ)(sibling(p).wait_recv)
        return 0

    lax.fori_loop(0, PAIRS, last, 0)


def kept(y, ref, k, c):
    for half in range(2):
        col = (half * (D // TN // 2) + k) * TN
        yield y.at[pl.ds(c * R, R), pl.ds(col, TN)], ref.at[half, pl.ds(k * R, R), :]


def copy_out(a, ra, rb, rc, o, buf, si, so, sk):
    n, r, steps = 4, 128, R // 128
    base = 3 * R

    def load(i):
        return pltpu.make_async_copy(a.at[pl.ds(base + i * r, r), :], buf.at[i % n], si.at[i % n])

    def store(i):
        return pltpu.make_async_copy(buf.at[i % n], o.at[pl.ds(base + i * r, r), :], so.at[i % n])

    for i in range(steps):
        load(i).start()
    whole = pltpu.make_async_copy(ra, o.at[pl.ds(0, R), :], sk.at[0])
    whole.start()
    for c, ref in ((1, rb), (2, rc)):
        for k in range(D // TN // 2):
            for dst, src in kept(o, ref, k, c):
                pltpu.make_async_copy(src, dst, sk.at[c]).start()
    for i in range(steps):
        load(i).wait()
        store(i).start()
    for i in range(steps):
        store(i).wait()
    whole.wait()
    for c in (1, 2):
        pltpu.make_async_copy(o.at[pl.ds(c * R, R), :], o.at[pl.ds(c * R, R), :], sk.at[c]).wait()


def solution(mesh):
    def step(x, w_gate, w_up, w_down):
        any_ = pl.BlockSpec(memory_space=pl.ANY)
        dma = pltpu.SemaphoreType.DMA
        vmem = pl.BlockSpec(memory_space=pltpu.VMEM)
        flops = 6 * ROWS * D * HID
        y, rows_a, rows_b, rows_c = pl.pallas_call(
            kernel,
            out_shape=(
                jax.ShapeDtypeStruct((ROWS, D), BF16),
                pltpu.VMEM((R, D), BF16),
                pltpu.VMEM((2, D, TN), BF16),
                pltpu.VMEM((2, D, TN), BF16),
            ),
            in_specs=[any_] * 4,
            out_specs=(any_, vmem, vmem, vmem),
            scratch_shapes=[
                pltpu.VMEM((2, R, HID), BF16),
                pltpu.VMEM((2, HID, CW), BF16),
                pltpu.VMEM((R, CW), BF16),
                pltpu.VMEM((2, R, CW), BF16),
                pltpu.VMEM((NS, R, CW), F32),
                pltpu.VMEM((NS, R, CW), BF16),
                pltpu.VMEM((NS, 2 * B, CW), BF16),
                pltpu.VMEM((NS, 2 * B, CW), BF16),
                pltpu.VMEM((NS, B, CW), BF16),
                pltpu.VMEM((NS, 4 * B, CW), BF16),
                pltpu.VMEM((NS, 2 * B, CW), BF16),
                pltpu.VMEM((NS, B, CW), BF16),
                dma((2,)),
                dma((2, 2)),
                dma((2,)),
                dma,
                dma((2,)),
                pltpu.SemaphoreType.REGULAR,
                dma((NS, 6)),
                dma((NS,)),
                dma((NS, 8)),
                dma((NS,)),
                dma((2, PAIRS)),
                dma((3,)),
            ],
            compiler_params=pltpu.CompilerParams(
                collective_id=0, has_side_effects=True, vmem_limit_bytes=38 << 20),
            cost_estimate=pl.CostEstimate(flops=flops, bytes_accessed=1 << 29, transcendentals=ROWS * HID),
            name="mlp",
        )(x, w_gate, w_up, w_down)
        return pl.pallas_call(
            copy_out,
            out_shape=jax.ShapeDtypeStruct((ROWS, D), BF16),
            in_specs=[any_, vmem, vmem, vmem],
            out_specs=any_,
            scratch_shapes=[pltpu.VMEM((4, 128, D), BF16), dma((4,)), dma((4,)), dma((3,))],
            compiler_params=pltpu.CompilerParams(vmem_limit_bytes=10 << 20),
            cost_estimate=pl.CostEstimate(flops=0, bytes_accessed=3 * ROWS * D, transcendentals=0),
            name="copy_out",
        )(y, rows_a, rows_b, rows_c)

    return jax.shard_map(
        step,
        mesh=mesh,
        in_specs=(P("dp", None), P(None, "tp"), P(None, "tp"), P("tp", None)),
        out_specs=P("dp", None),
        check_vma=False,
    )
```

```python
import jax
import jax.numpy as jnp
from jax import lax
from jax.experimental import pallas as pl
from jax.experimental.pallas import tpu as pltpu
from jax.sharding import PartitionSpec as P

ROWS, D, HID = 2048, 8192, 2048
R = 512
CW = 512
HALF = D // 2
NQ = HALF // CW
CHUNKS = ROWS // R
PAIRS = CHUNKS * NQ
TN = 256
UNITS = HID // TN
NS = 8
B = 64
SLOTS = 4
LEAD = UNITS
OFF = dict(Cm=29, B5m=20, A1e=3, B1m=7, A1m=8, A3e=15, A3m=20, B4m=20, B8e=22, Ce=28, B2m=11, A2m=13, A4e=22, B3m=14, B7e=16)
NIT = LEAD + PAIRS + max(OFF.values()) // SLOTS
KEEP = NIT - 7
F32, BF16 = jnp.float32, jnp.bfloat16


def kernel(x, wg, wu, wd, y, xb, gb, ub, hb, wdb, dsend, drecv, sf, sb, r_ya, r_oa, r_xa, r_ob, r_xb, r_yb,
           s_x, s_w, s_wd, s_ds, s_dr, credit, q_rs, q_send, q_final, q_leaf, q_sib, s_keep):
    dp, t = lax.axis_index("dp"), lax.axis_index("tp")
    core, z, yy = t % 2, (t // 2) % 4, t // 8
    s = z // 2
    mid = (z == 1) | (z == 2)
    end = (z == 0) | (z == 3)

    def tid(a, b, c):
        return (dp, (a * 4 + b) * 2 + c)

    to_y, to_x, to_s = tid(1 - yy, z, core), tid(yy, 3 - z, core), tid(yy, z, 1 - core)
    to_io = tid(yy, z + 1 - 2 * (z % 2), core)

    def rcopy(src, dst, ssem, rsem, dev):
        return pltpu.make_async_remote_copy(
            src_ref=src, dst_ref=dst, send_sem=ssem, recv_sem=rsem, device_id=dev, device_id_type=pl.DeviceIdType.MESH)

    bar = pltpu.get_barrier_semaphore()
    for dev in (to_y, to_io, to_s):
        pl.semaphore_signal(bar, inc=1, device_id=dev, device_id_type=pl.DeviceIdType.MESH)

    @pl.when(mid)
    def _():
        pl.semaphore_signal(bar, inc=1, device_id=to_x, device_id_type=pl.DeviceIdType.MESH)
        pl.semaphore_wait(bar, 4)

    @pl.when(end)
    def _():
        pl.semaphore_wait(bar, 3)

    def rows(r0, n):
        return pl.ds(pl.multiple_of(r0, B), n)

    def x_copy(c, i):
        h = R // 2
        return pltpu.make_async_copy(x.at[rows(c * R + i * h, h), :], xb.at[pl.ds(i * h, h), :], s_x.at[i])

    def w_copies(u):
        b, n = u % 2, pl.ds(pl.multiple_of((u % UNITS) * TN, TN), TN)
        return (pltpu.make_async_copy(wg.at[:, n], gb.at[b], s_w.at[b, 0]),
                pltpu.make_async_copy(wu.at[:, n], ub.at[b], s_w.at[b, 1]))

    def wd_copy(k, half, p):
        n = pl.ds(pl.multiple_of(half * HALF + (p % NQ) * CW, CW), CW)
        return pltpu.make_async_copy(wd.at[:, n], wdb.at[k], s_wd.at[k])

    def gate_up(u, i):
        b, n = u % 2, pl.ds(pl.multiple_of((u % UNITS) * TN, TN), TN)
        r = pl.ds(i * (R // 2), R // 2)
        g = jnp.dot(xb[r, :], gb[b], preferred_element_type=F32)
        up = jnp.dot(xb[r, :], ub[b], preferred_element_type=F32)
        hb[(u // UNITS) % 2, r, n] = (jax.nn.silu(g) * up).astype(BF16)

    def swap(q):
        return rcopy(dsend, drecv.at[q % 2], s_ds, s_dr.at[q % 2], to_s)

    def term_for_other(q):
        for j in range(1):
            n = pl.ds(j * CW, CW)
            dsend[:, n] = jnp.dot(hb[(q // NQ) % 2], wdb[0, :, n], preferred_element_type=F32).astype(BF16)

    def own_term(p, sl):
        for j in range(1):
            n = pl.ds(j * CW, CW)
            v = jnp.dot(hb[(p // NQ) % 2], wdb[1, :, n], preferred_element_type=F32) + drecv[p % 2, :, n].astype(F32)
            sf[sl, :, n] = v
            sb[sl, :, n] = v.astype(BF16)

    def add(sl, r0, n, srcs):
        w = 32
        def strip(i, _):
            v = sf[sl, pl.ds(pl.multiple_of(r0 + i * w, w), w), :]
            for ref, q0 in srcs:
                v = v + ref[sl, pl.ds(pl.multiple_of(q0 + i * w, w), w), :].astype(F32)
            sb[sl, pl.ds(pl.multiple_of(r0 + i * w, w), w), :] = v.astype(BF16)
            return 0
        lax.fori_loop(0, n // w, strip, 0, unroll=True)

    ya, oa, xa, ob, xbl, yb, ob2 = range(7)

    def reduce_copy(kind, sl, r0, n, dev):
        if kind in (ob, ob2):
            dst = r_ob.at[sl, rows((1 - s if kind == ob else s) * 2 * B, 2 * B), :]
        else:
            dst = (r_ya, r_oa, r_xa, None, r_xb, r_yb)[kind].at[sl]
        return rcopy(sb.at[sl, rows(r0, n), :], dst, q_send.at[sl], q_rs.at[sl, kind], dev)

    def y_at(p, r0, n):
        col = pl.multiple_of(core * HALF + (p % NQ) * CW, CW)
        return y.at[rows((p // NQ) * R + r0, n), pl.ds(col, CW)]

    def block_a(a, b):
        return (a * 2 + b) * B

    def block_b(b, a):
        return 256 + (b * 2 + a) * B

    def final_sem(sl, r0):
        return q_final.at[sl, r0 // B]

    def local_final(p, sl, r0):
        return pltpu.make_async_copy(sb.at[sl, rows(r0, B), :], y_at(p, r0, B), q_send.at[sl])

    def send_final(p, sl, r0, dev, leaf=False):
        sem = q_leaf.at[sl] if leaf else final_sem(sl, r0)
        return rcopy(sb.at[sl, rows(r0, B), :], y_at(p, r0, B), q_send.at[sl], sem, dev)

    def forward(p, sl, r0, dev, leaf=False):
        sem = q_leaf.at[sl] if leaf else final_sem(sl, r0)
        return rcopy(y_at(p, r0, B), y_at(p, r0, B), q_send.at[sl], sem, dev)

    def wait_blocks(sem, n):
        part = y.at[pl.ds(0, n * B), pl.ds(0, CW)]
        pltpu.make_async_copy(part, part, sem).wait()

    def sibling(p):
        return rcopy(y_at(p, 0, R), y_at(p, 0, R), q_sib.at[0, p], q_sib.at[1, p], to_s)

    def first(p, sl):
        reduce_copy(ya, sl, (1 - yy) * 128, 128, to_y).start()

        @pl.when(end)
        def _():
            reduce_copy(ob, sl, block_b(1 - s, 0), 128, to_io).start()
            reduce_copy(ob2, sl, block_b(s, 0), 128, to_io).start()

    def e_a1e(p, sl):
        reduce_copy(ya, sl, 0, 128, to_y).wait_recv()
        add(sl, yy * 128, 128, [(r_ya, 0)])
        reduce_copy(oa, sl, yy * 128, 128, to_io).start()

    def e_a1m(p, sl):
        reduce_copy(ya, sl, 0, 128, to_y).wait_recv()
        reduce_copy(oa, sl, 0, 128, to_io).wait_recv()
        add(sl, block_a(yy, 1 - s), B, [(r_ya, (1 - s) * B), (r_oa, (1 - s) * B)])
        reduce_copy(xa, sl, block_a(yy, 1 - s), B, to_x).start()

    def finals(p, sl, r0, leaf):
        send_final(p, sl, r0, to_x).start()
        send_final(p, sl, r0, to_io).start()
        send_final(p, sl, r0, to_y, leaf).start()
        local_final(p, sl, r0).start()

    def e_a2m(p, sl):
        reduce_copy(xa, sl, 0, B, to_x).wait_recv()
        add(sl, block_a(yy, s), B, [(r_ya, s * B), (r_oa, s * B), (r_xa, 0)])
        finals(p, sl, block_a(yy, s), True)

    def arrived(p, sl, r0):
        forward(p, sl, r0, to_y).wait_recv()

    def e_a3m(p, sl):
        r0 = block_a(yy, 1 - s)
        arrived(p, sl, r0)
        forward(p, sl, r0, to_io).start()
        forward(p, sl, r0, to_y, True).start()

    def pass_across(r0):
        def run(p, sl):
            arrived(p, sl, r0)
            forward(p, sl, r0, to_y, True).start()
        return run

    e_a3e, e_a4e = pass_across(block_a(yy, s)), pass_across(block_a(yy, 1 - s))
    e_b7e, e_b8e = pass_across(block_b(s, yy)), pass_across(block_b(1 - s, yy))

    def e_b1m(p, sl):
        reduce_copy(ob, sl, 256, 128, to_io).wait_recv()
        add(sl, block_b(1 - s, 0), 128, [(r_ob, (1 - s) * 128)])
        reduce_copy(xbl, sl, block_b(1 - s, 0), 128, to_x).start()

    def e_b2m(p, sl):
        reduce_copy(ob2, sl, 256, 128, to_io).wait_recv()
        reduce_copy(xbl, sl, 256, 128, to_x).wait_recv()
        add(sl, block_b(s, 1 - yy), B, [(r_ob, (s * 2 + 1 - yy) * B), (r_xb, (1 - yy) * B)])
        reduce_copy(yb, sl, block_b(s, 1 - yy), B, to_y).start()

    def e_b3m(p, sl):
        reduce_copy(yb, sl, 256, B, to_y).wait_recv()
        add(sl, block_b(s, yy), B, [(r_ob, (s * 2 + yy) * B), (r_xb, yy * B), (r_yb, 0)])
        finals(p, sl, block_b(s, yy), False)

    def e_b4m(p, sl):
        r0 = block_b(s, 1 - yy)
        arrived(p, sl, r0)
        forward(p, sl, r0, to_x, True).start()

    def e_b5m(p, sl):
        r0 = block_b(1 - s, yy)
        arrived(p, sl, r0)
        forward(p, sl, r0, to_io).start()

    def e_cm(p, sl):
        wait_blocks(q_leaf.at[sl], 3)
        wait_blocks(q_send.at[sl], 18)
        sibling(p).start()

    def e_ce(p, sl):
        wait_blocks(q_leaf.at[sl], 4)
        wait_blocks(q_send.at[sl], 12)
        sibling(p).start()

    events = dict(A1e=(end, e_a1e), A1m=(mid, e_a1m), A2m=(mid, e_a2m), A3m=(mid, e_a3m), A3e=(end, e_a3e), A4e=(end, e_a4e),
                  B1m=(mid, e_b1m), B2m=(mid, e_b2m), B3m=(mid, e_b3m), B4m=(mid, e_b4m), B5m=(mid, e_b5m), B7e=(end, e_b7e), B8e=(end, e_b8e),
                  Ce=(end, e_ce), Cm=(mid, e_cm))

    def comm(it, j):
        here = [(OFF[k], OFF[k] // SLOTS, *events[k]) for k in sorted(OFF, key=lambda k: -OFF[k]) if OFF[k] % SLOTS == j]
        if not here:
            return
        lags = [e[1] for e in here]
        steady = (it >= LEAD + max(lags)) & (it < LEAD + PAIRS + min(lags))

        def run_all(role, guarded):
            for _, lag, of, run in here:
                if of is not role:
                    continue
                p = it - LEAD - lag
                if guarded:
                    pl.when((p >= 0) & (p < PAIRS))(lambda run=run, p=p: run(p, p % NS))
                else:
                    run(p, p % NS)

        def both(guarded):
            lax.cond(mid, lambda: run_all(mid, guarded), lambda: run_all(end, guarded))

        lax.cond(steady, lambda: both(False), lambda: both(True))

    x_copy(0, 0).start()
    for c in w_copies(0):
        c.start()
    x_copy(0, 1).start()

    def other_half(q):
        wd_copy(0, 0, 0).wait()
        pl.when(q >= 1)(lambda: swap(q - 1).wait_send())
        term_for_other(q)
        pl.when(q >= 2)(lambda: pl.semaphore_wait(credit, 1))
        swap(q).start()
        pl.when(q + 1 < PAIRS)(lambda: wd_copy(0, 1 - core, q + 1).start())

    def landed(p, _):
        sibling(p).wait_recv()
        return 0

    def body(it, _):
        p, q = it - LEAD, it - LEAD + 1

        @pl.when(it == KEEP)
        def _():
            lax.fori_loop(0, 3 * NQ, landed, 0)
            pltpu.make_async_copy(y.at[pl.ds(0, R), :], xb, s_keep.at[0]).start()
            for c, ref in ((1, gb), (2, ub)):
                for k in range(D // TN // 2):
                    for src, dst in kept(y, ref, k, c):
                        pltpu.make_async_copy(src, dst, s_keep.at[c]).start()


        @pl.when((p >= 0) & (p < PAIRS))
        def _():
            wd_copy(1, 0, 0).wait()
            swap(p).wait_recv()
            own_term(p, p % NS)

            @pl.when(p < PAIRS - 2)
            def _():
                pl.semaphore_signal(credit, inc=1, device_id=to_s, device_id_type=pl.DeviceIdType.MESH)
            first(p, p % NS)
            pl.when(p + 1 < PAIRS)(lambda: wd_copy(1, core, p + 1).start())
        comm(it, 0)
        pl.when((q >= 1) & (q < PAIRS) & (q % NQ != 0))(lambda: other_half(q))
        comm(it, 1)
        for i in range(2):
            @pl.when(it < PAIRS)
            def _():
                pl.when(it % UNITS == 0)(x_copy(0, i).wait)
                if i == 0:
                    for c in w_copies(it):
                        c.wait()

                    @pl.when(it + 1 < PAIRS)
                    def _():
                        for c in w_copies(it + 1):
                            c.start()

                    @pl.when(it == 0)
                    def _():
                        wd_copy(0, 1 - core, 0).start()
                        wd_copy(1, core, 0).start()
                gate_up(it, i)
                pl.when((it % UNITS == UNITS - 1) & (it < PAIRS - 1))(lambda: x_copy(it // UNITS + 1, i).start())
            comm(it, 2 + i)
        pl.when((q >= 0) & (q < PAIRS) & (q % NQ == 0))(lambda: other_half(q))
        return 0

    lax.fori_loop(0, NIT, body, 0)
    swap(PAIRS - 1).wait_send()

    pltpu.make_async_copy(y.at[pl.ds(0, R), :], xb, s_keep.at[0]).wait()
    for c in (1, 2):
        pltpu.make_async_copy(y.at[pl.ds(c * R, R), :], y.at[pl.ds(c * R, R), :], s_keep.at[c]).wait()

    def last(p, _):
        sibling(p).wait_send()
        pl.when(p >= 3 * NQ)(sibling(p).wait_recv)
        return 0

    lax.fori_loop(0, PAIRS, last, 0)


def kept(y, ref, k, c):
    for half in range(2):
        col = (half * (D // TN // 2) + k) * TN
        yield y.at[pl.ds(c * R, R), pl.ds(col, TN)], ref.at[half, pl.ds(k * R, R), :]


def copy_out(a, ra, rb, rc, o, buf, si, so, sk):
    n, r, steps = 4, 128, R // 128
    base = 3 * R

    def load(i):
        return pltpu.make_async_copy(a.at[pl.ds(base + i * r, r), :], buf.at[i % n], si.at[i % n])

    def store(i):
        return pltpu.make_async_copy(buf.at[i % n], o.at[pl.ds(base + i * r, r), :], so.at[i % n])

    for i in range(steps):
        load(i).start()
    whole = pltpu.make_async_copy(ra, o.at[pl.ds(0, R), :], sk.at[0])
    whole.start()
    for c, ref in ((1, rb), (2, rc)):
        for k in range(D // TN // 2):
            for dst, src in kept(o, ref, k, c):
                pltpu.make_async_copy(src, dst, sk.at[c]).start()
    for i in range(steps):
        load(i).wait()
        store(i).start()
    for i in range(steps):
        store(i).wait()
    whole.wait()
    for c in (1, 2):
        pltpu.make_async_copy(o.at[pl.ds(c * R, R), :], o.at[pl.ds(c * R, R), :], sk.at[c]).wait()


def solution(mesh):
    def step(x, w_gate, w_up, w_down):
        any_ = pl.BlockSpec(memory_space=pl.ANY)
        dma = pltpu.SemaphoreType.DMA
        vmem = pl.BlockSpec(memory_space=pltpu.VMEM)
        flops = 6 * ROWS * D * HID
        y, rows_a, rows_b, rows_c = pl.pallas_call(
            kernel,
            out_shape=(
                jax.ShapeDtypeStruct((ROWS, D), BF16),
                pltpu.VMEM((R, D), BF16),
                pltpu.VMEM((2, D, TN), BF16),
                pltpu.VMEM((2, D, TN), BF16),
            ),
            in_specs=[any_] * 4,
            out_specs=(any_, vmem, vmem, vmem),
            scratch_shapes=[
                pltpu.VMEM((2, R, HID), BF16),
                pltpu.VMEM((2, HID, CW), BF16),
                pltpu.VMEM((R, CW), BF16),
                pltpu.VMEM((2, R, CW), BF16),
                pltpu.VMEM((NS, R, CW), F32),
                pltpu.VMEM((NS, R, CW), BF16),
                pltpu.VMEM((NS, 2 * B, CW), BF16),
                pltpu.VMEM((NS, 2 * B, CW), BF16),
                pltpu.VMEM((NS, B, CW), BF16),
                pltpu.VMEM((NS, 4 * B, CW), BF16),
                pltpu.VMEM((NS, 2 * B, CW), BF16),
                pltpu.VMEM((NS, B, CW), BF16),
                dma((2,)),
                dma((2, 2)),
                dma((2,)),
                dma,
                dma((2,)),
                pltpu.SemaphoreType.REGULAR,
                dma((NS, 7)),
                dma((NS,)),
                dma((NS, 8)),
                dma((NS,)),
                dma((2, PAIRS)),
                dma((3,)),
            ],
            compiler_params=pltpu.CompilerParams(
                collective_id=0, has_side_effects=True, vmem_limit_bytes=38 << 20),
            cost_estimate=pl.CostEstimate(flops=flops, bytes_accessed=1 << 29, transcendentals=ROWS * HID),
            name="mlp",
        )(x, w_gate, w_up, w_down)
        return pl.pallas_call(
            copy_out,
            out_shape=jax.ShapeDtypeStruct((ROWS, D), BF16),
            in_specs=[any_, vmem, vmem, vmem],
            out_specs=any_,
            scratch_shapes=[pltpu.VMEM((4, 128, D), BF16), dma((4,)), dma((4,)), dma((3,))],
            compiler_params=pltpu.CompilerParams(vmem_limit_bytes=10 << 20),
            cost_estimate=pl.CostEstimate(flops=0, bytes_accessed=3 * ROWS * D, transcendentals=0),
            name="copy_out",
        )(y, rows_a, rows_b, rows_c)

    return jax.shard_map(
        step,
        mesh=mesh,
        in_specs=(P("dp", None), P(None, "tp"), P(None, "tp"), P("tp", None)),
        out_specs=P("dp", None),
        check_vma=False,
    )
```
